32 devices in a mesh: groups: 2 (over y), feat: 4 (over x, core), loop: 4 (over z).
Axes of the slice: x: 2, y: 2, z: 4, core: 2. Of those that a mesh axis runs over, the one named last changes fastest.
Arguments:
- train_grads: bfloat16 [512, 65536], P(('groups', 'loop'), 'feat'), parts along dimension 0, may hold values from -6 to 6
- query_grads: bfloat16 [64, 65536], P(('groups', 'loop'), 'feat'), parts along dimension 0, may hold values from -0.0234375 to 0.0234375
- curvature: float32 [65536], P('feat'), may hold values from 0.05 to 5
- row_counts: int32 [8], P(('groups', 'loop')), parts along dimension 0, may hold values from 1 to 64, 128 in all
Outputs:
- scores: float32 [512, 32], P(('groups', 'loop', 'feat')), parts along dimension 0
The draws below stay inside these ranges and needn't reach their ends.
There are 2 independent parts, one for each index of `groups`. The reference program is written for one: setup_inputs(seed, part) draws one part's arguments, and reference() takes and returns one part's arrays. A program takes and returns all parts, laid end to end along the dimension named above; an argument that names none is the same for every part. Nothing has to cross between parts.
Inputs may be any that keep to these rules, and one draw needn't show every extreme that they name: row_counts[s] is the number of live slots of loop shard s; slots 0 to row_counts[s] - 1 of that shard are live; some shard has exactly 64; the counts sum to 128.
All inputs are finite; a program needn't handle non-finite values.
Results may differ from the reference program's by a relative error of at most 0.0029.
Values may be sent and summed in bfloat16 or wider, within the bound.
A program may use at most 128 MiB of HBM per device.

```python
import math
import jax
import jax.numpy as jnp
import numpy as np

F = 65536
CAP = 64
TRAIN = 256
QUERIES = 32
N_LOOP = 4


def level_of(key, shape, split, low, top_value):
    loudness, own = 1.0, jax.random.fold_in(key, 6)
    for axis_at, parts in split:
        draws = jnp.exp(jax.random.uniform(jax.random.fold_in(own, axis_at), (parts,), jnp.float32, low / len(split), top_value / len(split)))
        loudness = loudness * jnp.repeat(draws, shape[axis_at] // parts).reshape([-1 if axis == axis_at else 1 for axis in range(len(shape))])
    return loudness


def profile(number_of, total, reach, lean):
    weights = [(1 << 20) // math.isqrt(grade ** lean) + 1 for grade in range(2, number_of + 1)]
    rest, counts = total - reach - (number_of - 1), [1] * (number_of - 1)
    while rest > 0:
        movable = [i for i in range(number_of - 1) if counts[i] < reach]
        mass, left = sum([weights[i] for i in movable]), rest
        for i in movable:
            addition = min(reach - counts[i], max(1, left * weights[i] // mass), rest)
            counts[i] = counts[i] + addition
            rest = rest - addition
    return np.array([reach] + counts)


def ragged_sizes(stream_key, count, total, reach, lean):
    if count == 2:
        one = jax.random.randint(stream_key, (), max(1, total - reach), min(reach, total - 1) + 1)
        return jnp.stack([one, total - one])
    tallies = jnp.asarray(profile(count, total, reach, lean), jnp.int32)
    pairs = (count - 1) // 2
    giver, receiver = tallies[1:1 + 2 * pairs:2], tallies[2:2 + 2 * pairs:2]
    room = jnp.minimum(giver - 1, reach - receiver)
    shifted = jax.random.randint(jax.random.fold_in(stream_key, 1), (pairs,), 0, 1 << 20) % (room + 1)
    tallies = tallies.at[1:1 + 2 * pairs:2].set(giver - shifted).at[2:2 + 2 * pairs:2].set(receiver + shifted)
    return tallies[jax.random.permutation(jax.random.fold_in(stream_key, 2), count)]


def bell_draw(own_key, dims, spread, bound, shards=(), kind=jnp.bfloat16):
    drawn = jax.random.normal(own_key, dims, jnp.float32) * spread
    if len(shards) > 0:
        drawn = level_of(own_key, dims, shards, -0.22, 0.18) * drawn
    return jnp.clip(drawn, min=-bound, max=bound).astype(kind)


def setup_inputs(seed: int = 0, part: int = 0) -> dict:
    key_of = jax.random.split(jax.random.key(seed), 5)
    part_keys = jax.random.split(jax.random.fold_in(key_of[4], part), 5)
    return {
        "train_grads": bell_draw(part_keys[0], (TRAIN, F), 1.0, 6.0, ((0, 4), (1, 4))),
        "query_grads": bell_draw(part_keys[1], (QUERIES, F), F ** -0.5, 0.0234375, ((0, 4), (1, 4))),
        "curvature": jnp.clip(jnp.exp(math.log(5.0) - 4.6051702 * jax.random.uniform(key_of[2], (F,), jnp.float32) ** level_of(key_of[2], (F,), ((0, 4),), -0.2, 0.2)), 0.05, 5.0),
        "row_counts": ragged_sizes(part_keys[3], N_LOOP, N_LOOP * CAP // 2, CAP, 2).astype(jnp.int32),
    }


damping_term = 0.1


def reference(train_grads, query_grads, curvature, row_counts):
    precond = (query_grads.astype(jnp.float32) / (damping_term + curvature[None, :])).astype(jnp.bfloat16)
    slots = jnp.arange(TRAIN, dtype=jnp.int32)
    shard_of = (slots // CAP).astype(jnp.int32)
    live = (slots % CAP) < row_counts[shard_of]
    raw = jnp.dot(train_grads, precond.T, preferred_element_type=jnp.float32)
    return jnp.where(live[:, None], raw, jnp.float32(0.0))
```

```python
import functools

import jax
import jax.numpy as jnp
from jax import lax
from jax.experimental import pallas as pl
from jax.experimental.pallas import tpu as pltpu
from jax.sharding import PartitionSpec as P

MESH = pl.DeviceIdType.MESH
damping_term = 0.1


def kernel(
    n, nf, pieces,
    t_hbm, q_hbm, c_hbm, count_hbm, out_ref,
    gath, t_ref, count_ref, c_ref, inv_ref, acc, part, red,
    local_sem, recv_sem, send_sem, red_recv, red_send,
):
    me, f = lax.axis_index("loop"), lax.axis_index("feat")
    rows, width = t_ref.shape
    own_rows = rows // nf
    q_rows = gath.shape[1]
    cols = width // pieces
    has_left, has_right = me > 0, me < n - 1

    load_q = pltpu.make_async_copy(q_hbm, gath.at[me], local_sem.at[0])
    load_c = pltpu.make_async_copy(c_hbm, c_ref, local_sem.at[1])
    load_t = pltpu.make_async_copy(t_hbm, t_ref, local_sem.at[2])
    load_count = pltpu.make_async_copy(count_hbm, count_ref, local_sem.at[3])
    load_q.start()

    barrier = pltpu.get_barrier_semaphore()

    @pl.when(has_left)
    def _():
        pl.semaphore_signal(barrier, inc=1, device_id={"loop": me - 1}, device_id_type=MESH)

    @pl.when(has_right)
    def _():
        pl.semaphore_signal(barrier, inc=1, device_id={"loop": me + 1}, device_id_type=MESH)

    for k in range(1, nf):
        pl.semaphore_signal(
            barrier, inc=1, device_id={"feat": lax.rem(f + k, nf)}, device_id_type=MESH
        )
    load_c.start()
    load_t.start()
    load_count.start()

    def hop(way, block, piece):
        span = gath.at[block, :, pl.ds(pl.multiple_of(piece * cols, 128), cols)]
        return pltpu.make_async_remote_copy(
            src_ref=span,
            dst_ref=span,
            send_sem=send_sem.at[way, block * pieces + piece],
            recv_sem=recv_sem.at[block * pieces + piece],
            device_id={"loop": jnp.clip(me + (2 * way - 1), 0, n - 1)},
            device_id_type=MESH,
        )

    def multiply(block, piece):
        at = pl.ds(pl.multiple_of(piece * cols, 128), cols)
        scaled = (gath[block, :, at].astype(jnp.float32) * inv_ref[:, at]).astype(jnp.bfloat16)
        here = pl.ds(pl.multiple_of(block * q_rows, q_rows), q_rows)
        acc[here, 0:rows] += lax.dot_general(
            scaled, t_ref[:, at], (((1,), (1,)), ((), ())), preferred_element_type=jnp.float32
        )

    acc[...] = jnp.zeros_like(acc)
    load_q.wait()
    pl.semaphore_wait(barrier, has_left.astype(jnp.int32) + has_right.astype(jnp.int32) + nf - 1)

    for piece in range(pieces):
        @pl.when(has_right)
        def _(piece=piece):
            hop(1, me, piece).start()

        @pl.when(has_left)
        def _(piece=piece):
            hop(0, me, piece).start()

    load_c.wait()
    inv_ref[...] = 1.0 / (damping_term + c_ref[...])
    load_t.wait()

    @pl.loop(0, pieces)
    def _(piece):
        multiply(me, piece)

    @pl.loop(0, (n - 1) * pieces)
    def _(step):
        back, piece = step // pieces + 1, lax.rem(step, pieces)
        from_left, from_right = me - back, me + back

        @pl.when(from_left >= 0)
        def _():
            hop(1, from_left, piece).wait_recv()

            @pl.when(has_right)
            def _():
                hop(1, from_left, piece).start()

        @pl.when(from_right < n)
        def _():
            hop(0, from_right, piece).wait_recv()

            @pl.when(has_left)
            def _():
                hop(0, from_right, piece).start()

        @pl.when(from_left >= 0)
        def _():
            multiply(from_left, piece)

        @pl.when(from_right < n)
        def _():
            multiply(from_right, piece)

    turned = acc[...].T
    for k in range(nf):
        part[k] = turned[k * own_rows:(k + 1) * own_rows, 0:part.shape[2]]

    shares = []
    for k in range(1, nf):
        peer = lax.rem(f + k, nf)
        share = pltpu.make_async_remote_copy(
            src_ref=part.at[peer],
            dst_ref=red.at[k - 1],
            send_sem=red_send.at[k - 1],
            recv_sem=red_recv.at[k - 1],
            device_id={"feat": peer},
            device_id_type=MESH,
        )
        share.start()
        shares.append(share)

    @pl.loop(0, n * pieces)
    def _(at):
        block, piece = at // pieces, lax.rem(at, pieces)

        @pl.when(has_right & (block <= me))
        def _():
            hop(1, block, piece).wait_send()

        @pl.when(has_left & (block >= me))
        def _():
            hop(0, block, piece).wait_send()

    load_count.wait()
    slot = f * own_rows + lax.broadcasted_iota(jnp.int32, out_ref.shape, 0)
    total = part[f]
    for k in range(1, nf):
        shares[k - 1].wait_recv()
        total = total + red[k - 1]
    out_ref[...] = jnp.where(slot < count_ref[0], total, 0.0)
    for share in shares:
        share.wait_send()


def on_device(n, nf, train_grads, query_grads, curvature, row_counts):
    rows, width = train_grads.shape
    q_rows = query_grads.shape[0]
    queries = n * q_rows
    pieces = max(1, 16 // n)
    padded = -(-queries // 128) * 128
    lanes = -(-rows // 128) * 128
    hbm = pl.BlockSpec(memory_space=pl.ANY)
    return pl.pallas_call(
        functools.partial(kernel, n, nf, pieces),
        out_shape=jax.ShapeDtypeStruct((rows // nf, queries), jnp.float32),
        in_specs=[hbm] * 4,
        out_specs=pl.BlockSpec(memory_space=pltpu.VMEM),
        scratch_shapes=[
            pltpu.VMEM((n, q_rows, width), jnp.bfloat16),
            pltpu.VMEM((rows, width), jnp.bfloat16),
            pltpu.SMEM((1,), jnp.int32),
            pltpu.VMEM((1, width), jnp.float32),
            pltpu.VMEM((1, width), jnp.float32),
            pltpu.VMEM((padded, lanes), jnp.float32),
            pltpu.VMEM((nf, rows // nf, queries), jnp.float32),
            pltpu.VMEM((nf - 1, rows // nf, queries), jnp.float32),
            pltpu.SemaphoreType.DMA((4,)),
            pltpu.SemaphoreType.DMA((n * pieces,)),
            pltpu.SemaphoreType.DMA((2, n * pieces)),
            pltpu.SemaphoreType.DMA((nf - 1,)),
            pltpu.SemaphoreType.DMA((nf - 1,)),
        ],
        compiler_params=pltpu.CompilerParams(collective_id=0, has_side_effects=True),
    )(train_grads, query_grads, curvature.reshape(1, width), row_counts)


def solution(mesh):
    placed = (
        P(("groups", "loop"), "feat"),
        P(("groups", "loop"), "feat"),
        P("feat"),
        P(("groups", "loop")),
    )
    return jax.shard_map(
        functools.partial(on_device, mesh.shape["loop"], mesh.shape["feat"]),
        mesh=mesh,
        in_specs=placed,
        out_specs=P(("groups", "loop", "feat"), None),
        check_vma=False,
    )
```

```python
import functools
import math

import jax
import jax.numpy as jnp
from jax import lax
from jax.experimental import pallas as pl
from jax.experimental.pallas import tpu as pltpu
from jax.sharding import PartitionSpec as P

MESH = pl.DeviceIdType.MESH
damping_term = 0.1


def kernel(
    n, nf, pieces, tail,
    t_hbm, q_hbm, c_hbm, count_hbm, out_ref,
    gath, t_ref, count_ref, c_ref, inv_ref, acc, part, red, t_tail, p_tail, tail_acc, tail_part, tail_red,
    local_sem, recv_sem, send_sem, red_recv, red_send, give_sem, tail_recv, tail_send,
):
    me, f = lax.axis_index("loop"), lax.axis_index("feat")
    rows, width = t_ref.shape
    own_rows = rows // nf
    q_rows = gath.shape[1]
    main = width - tail
    cols = main // pieces
    stride = pieces + 1
    has_left, has_right = me > 0, me < n - 1
    is_end = (me == 0) | (me == n - 1)
    is_helper = (me == 1) | (me == n - 2)

    load_q = pltpu.make_async_copy(q_hbm, gath.at[me], local_sem.at[0])
    load_c = pltpu.make_async_copy(c_hbm, c_ref, local_sem.at[1])
    load_t = pltpu.make_async_copy(t_hbm, t_ref, local_sem.at[2])
    load_count = pltpu.make_async_copy(count_hbm, count_ref, local_sem.at[3])
    load_q.start()

    barrier = pltpu.get_barrier_semaphore()

    @pl.when(has_left)
    def _():
        pl.semaphore_signal(barrier, inc=1, device_id={"loop": me - 1}, device_id_type=MESH)

    @pl.when(has_right)
    def _():
        pl.semaphore_signal(barrier, inc=1, device_id={"loop": me + 1}, device_id_type=MESH)

    for k in range(1, nf):
        pl.semaphore_signal(
            barrier, inc=1, device_id={"feat": lax.rem(f + k, nf)}, device_id_type=MESH
        )
    load_c.start()
    load_t.start()
    load_count.start()

    def columns(piece):
        if piece is None:
            return pl.ds(main, tail)
        return pl.ds(pl.multiple_of(piece * cols, 128), cols)

    def hop(way, block, piece):
        span = gath.at[block, :, columns(piece)]
        at = block * stride + (pieces if piece is None else piece)
        return pltpu.make_async_remote_copy(
            src_ref=span,
            dst_ref=span,
            send_sem=send_sem.at[way, at],
            recv_sem=recv_sem.at[at],
            device_id={"loop": jnp.clip(me + (2 * way - 1), 0, n - 1)},
            device_id_type=MESH,
        )

    def goes_right(piece):
        return has_right if piece is not None else me < n - 2

    def goes_left(piece):
        return has_left if piece is not None else me > 1

    def multiply(block, piece):
        at = columns(piece)
        exact = gath[block, :, at].astype(jnp.float32) * inv_ref[:, at]
        here = pl.ds(pl.multiple_of(block * q_rows, q_rows), q_rows)
        acc[here, 0:rows] += lax.dot_general(
            exact.astype(jnp.bfloat16), t_ref[:, at], (((1,), (1,)), ((), ())),
            preferred_element_type=jnp.float32,
        )
        if piece is None:
            p_tail[here, :] = exact

    def send_own(piece):
        @pl.when(goes_right(piece))
        def _():
            hop(1, me, piece).start()

        @pl.when(goes_left(piece))
        def _():
            hop(0, me, piece).start()

    def arrive(back, piece):
        from_left, from_right = me - back, me + back
        takes_left, takes_right = from_left >= 0, from_right < n
        if piece is None:
            takes_left, takes_right = takes_left & has_right, takes_right & has_left

        @pl.when(takes_left)
        def _():
            hop(1, from_left, piece).wait_recv()

            @pl.when(goes_right(piece))
            def _():
                hop(1, from_left, piece).start()

        @pl.when(takes_right)
        def _():
            hop(0, from_right, piece).wait_recv()

            @pl.when(goes_left(piece))
            def _():
                hop(0, from_right, piece).start()

        @pl.when(takes_left)
        def _():
            multiply(from_left, piece)

        @pl.when(takes_right)
        def _():
            multiply(from_right, piece)

    give = pltpu.make_async_remote_copy(
        src_ref=t_ref.at[:, pl.ds(main, t_tail.shape[1])],
        dst_ref=t_tail,
        send_sem=give_sem.at[0],
        recv_sem=give_sem.at[1],
        device_id={"loop": jnp.where(me == 0, 1, n - 2)},
        device_id_type=MESH,
    ) if tail else None

    acc[...] = jnp.zeros_like(acc)
    load_q.wait()
    pl.semaphore_wait(barrier, has_left.astype(jnp.int32) + has_right.astype(jnp.int32) + nf - 1)

    for piece in range(pieces):
        send_own(piece)
    load_t.wait()
    if tail:
        send_own(None)

        @pl.when(is_end)
        def _():
            give.start()

    load_c.wait()
    inv_ref[...] = 1.0 / (damping_term + c_ref[...])

    @pl.loop(0, pieces)
    def _(piece):
        multiply(me, piece)

    if tail:
        @pl.when(jnp.logical_not(is_end))
        def _():
            multiply(me, None)

    @pl.loop(1, n)
    def _(back):
        @pl.loop(0, pieces)
        def _(piece):
            arrive(back, piece)

        if tail:
            arrive(back, None)

    turned = acc[...].T
    for k in range(nf):
        part[k] = turned[k * own_rows:(k + 1) * own_rows, 0:part.shape[2]]

    shares = []
    for k in range(1, nf):
        peer = lax.rem(f + k, nf)
        share = pltpu.make_async_remote_copy(
            src_ref=part.at[peer],
            dst_ref=red.at[k - 1],
            send_sem=red_send.at[k - 1],
            recv_sem=red_recv.at[k - 1],
            device_id={"feat": peer},
            device_id_type=MESH,
        )
        share.start()
        shares.append(share)

    tail_shares = []
    if tail:
        for k in range(nf):
            peer = lax.rem(f + k, nf)
            tail_shares.append(pltpu.make_async_remote_copy(
                src_ref=tail_part.at[peer],
                dst_ref=tail_red.at[k],
                send_sem=tail_send.at[k],
                recv_sem=tail_recv.at[k],
                device_id={"feat": peer, "loop": jnp.where(me == 1, 0, n - 1)},
                device_id_type=MESH,
            ))

        @pl.when(is_helper)
        def _():
            give.wait_recv()
            tail_acc[...] = jnp.zeros_like(tail_acc)
            wide = math.gcd(tail, 512)

            @pl.loop(0, tail // wide)
            def _(step):
                at = pl.ds(pl.multiple_of(step * wide, 128), wide)
                tail_acc[...] += lax.dot_general(
                    t_tail[:, at], p_tail[:, at].astype(jnp.bfloat16), (((1,), (1,)), ((), ())),
                    preferred_element_type=jnp.float32,
                )

            for k in range(nf):
                tail_part[k] = tail_acc[k * own_rows:(k + 1) * own_rows, :]
            for share in tail_shares:
                share.start()

    @pl.loop(0, n)
    def _(block):
        for piece in [*range(pieces), None][:pieces + (tail > 0)]:
            @pl.when(goes_right(piece) & (block <= me))
            def _():
                hop(1, block, piece).wait_send()

            @pl.when(goes_left(piece) & (block >= me))
            def _():
                hop(0, block, piece).wait_send()

    load_count.wait()
    live = f * own_rows + lax.broadcasted_iota(jnp.int32, out_ref.shape, 0) < count_ref[0]
    total = part[f]
    for k in range(1, nf):
        shares[k - 1].wait_recv()
        total = total + red[k - 1]
    out_ref[...] = jnp.where(live, total, 0.0)
    if tail:
        @pl.when(is_end)
        def _():
            more = jnp.zeros_like(total)
            for k in range(nf):
                tail_shares[k].wait_recv()
                more = more + tail_red[k]
            out_ref[...] = jnp.where(live, total + more, 0.0)
            give.wait_send()

        @pl.when(is_helper)
        def _():
            for share in tail_shares:
                share.wait_send()
    for share in shares:
        share.wait_send()


def on_device(n, nf, train_grads, query_grads, curvature, row_counts):
    rows, width = train_grads.shape
    q_rows = query_grads.shape[0]
    queries = n * q_rows
    pieces = max(1, 16 // n)
    unit = 128 * pieces
    tail = width - width * 26 // 32 // unit * unit if n >= 4 else 0
    padded = -(-queries // 128) * 128
    lanes = -(-rows // 128) * 128
    hbm = pl.BlockSpec(memory_space=pltpu.HBM)
    return pl.pallas_call(
        functools.partial(kernel, n, nf, pieces, tail),
        out_shape=pltpu.VMEM((rows // nf, queries), jnp.float32),
        in_specs=[hbm] * 4,
        out_specs=pl.BlockSpec(memory_space=pltpu.VMEM),
        scratch_shapes=[
            pltpu.VMEM((n, q_rows, width), jnp.bfloat16),
            pltpu.VMEM((rows, width), jnp.bfloat16),
            pltpu.SMEM((1,), jnp.int32),
            pltpu.VMEM((1, width), jnp.float32),
            pltpu.VMEM((1, width), jnp.float32),
            pltpu.VMEM((padded, lanes), jnp.float32),
            pltpu.VMEM((nf, rows // nf, queries), jnp.float32),
            pltpu.VMEM((nf - 1, rows // nf, queries), jnp.float32),
            pltpu.VMEM((rows, tail or 128), jnp.bfloat16),
            pltpu.VMEM((queries, tail or 128), jnp.float32),
            pltpu.VMEM((rows, queries), jnp.float32),
            pltpu.VMEM((nf, rows // nf, queries), jnp.float32),
            pltpu.VMEM((nf, rows // nf, queries), jnp.float32),
            pltpu.SemaphoreType.DMA((4,)),
            pltpu.SemaphoreType.DMA((n * (pieces + 1),)),
            pltpu.SemaphoreType.DMA((2, n * (pieces + 1))),
            pltpu.SemaphoreType.DMA((nf - 1,)),
            pltpu.SemaphoreType.DMA((nf - 1,)),
            pltpu.SemaphoreType.DMA((2,)),
            pltpu.SemaphoreType.DMA((nf,)),
            pltpu.SemaphoreType.DMA((nf,)),
        ],
        compiler_params=pltpu.CompilerParams(collective_id=0, has_side_effects=True),
    )(train_grads, query_grads, curvature.reshape(1, width), row_counts)


def solution(mesh):
    placed = (
        P(("groups", "loop"), "feat"),
        P(("groups", "loop"), "feat"),
        P("feat"),
        P(("groups", "loop")),
    )
    return jax.shard_map(
        functools.partial(on_device, mesh.shape["loop"], mesh.shape["feat"]),
        mesh=mesh,
        in_specs=placed,
        out_specs=P(("groups", "loop", "feat"), None),
        check_vma=False,
    )
```

```python
import functools
import math

import jax
import jax.numpy as jnp
from jax import lax
from jax.experimental import pallas as pl
from jax.experimental.pallas import tpu as pltpu
from jax.sharding import PartitionSpec as P

MESH = pl.DeviceIdType.MESH
damping_term = 0.1


def kernel(
    n, nf, pieces, tail,
    t_hbm, q_hbm, c_hbm, count_hbm, out_ref,
    gath, t_ref, count_ref, c_ref, inv_ref, acc, part, red, t_tail, p_tail, tail_acc, tail_part, tail_red,
    local_sem, recv_sem, send_sem, red_recv, red_send, give_sem, tail_recv, tail_send, ready_sem,
):
    me, f = lax.axis_index("loop"), lax.axis_index("feat")
    rows, width = t_ref.shape
    own_rows = rows // nf
    q_rows = gath.shape[1]
    main = width - tail
    cols = main // pieces
    stride = pieces + 1
    has_left, has_right = me > 0, me < n - 1
    is_end = (me == 0) | (me == n - 1)
    is_helper = (me == 1) | (me == n - 2)

    load_q = pltpu.make_async_copy(q_hbm, gath.at[me], local_sem.at[0])
    load_c = pltpu.make_async_copy(c_hbm, c_ref, local_sem.at[1])
    load_t = pltpu.make_async_copy(t_hbm, t_ref, local_sem.at[2])
    load_count = pltpu.make_async_copy(count_hbm, count_ref, local_sem.at[3])
    load_q.start()

    barrier = pltpu.get_barrier_semaphore()

    @pl.when(has_right)
    def _():
        pl.semaphore_signal(barrier, inc=1, device_id={"loop": me + 1}, device_id_type=MESH)

    for k in range(1, nf):
        pl.semaphore_signal(
            barrier, inc=1, device_id={"feat": lax.rem(f + k, nf)}, device_id_type=MESH
        )
    load_c.start()
    load_t.start()
    load_count.start()

    def columns(piece):
        if piece is None:
            return pl.ds(main, tail)
        return pl.ds(pl.multiple_of(piece * cols, 128), cols)

    def hop(way, block, piece):
        span = gath.at[block, :, columns(piece)]
        at = block * stride + (pieces if piece is None else piece)
        return pltpu.make_async_remote_copy(
            src_ref=span,
            dst_ref=span,
            send_sem=send_sem.at[way, at],
            recv_sem=recv_sem.at[at],
            device_id={"loop": jnp.clip(me + (2 * way - 1), 0, n - 1)},
            device_id_type=MESH,
        )

    def goes_right(piece):
        return has_right if piece is not None else me < n - 2

    def goes_left(piece):
        return has_left if piece is not None else me > 1

    def multiply(block, piece):
        start, size = (main, tail) if piece is None else (piece * cols, cols)
        here = pl.ds(pl.multiple_of(block * q_rows, q_rows), q_rows)
        wide = size // 2 if size % 256 == 0 else size

        @pl.loop(0, size // wide)
        def _(step):
            at = pl.ds(pl.multiple_of(start + step * wide, 128), wide)
            exact = gath[block, :, at].astype(jnp.float32) * inv_ref[:, at]
            acc[here, 0:rows] += lax.dot_general(
                exact.astype(jnp.bfloat16), t_ref[:, at], (((1,), (1,)), ((), ())),
                preferred_element_type=jnp.float32,
            )
            if piece is None:
                p_tail[here, pl.ds(pl.multiple_of(step * wide, 128), wide)] = exact

    def arrive(back, piece):
        from_left, from_right = me - back, me + back
        takes_left, takes_right = from_left >= 0, from_right < n
        if piece is None:
            inner = jnp.logical_not(is_end)
            takes_left, takes_right = takes_left & inner, takes_right & inner
        moved = back > 0

        @pl.when(takes_left & moved)
        def _():
            hop(1, from_left, piece).wait_recv()

            @pl.when(goes_right(piece))
            def _():
                hop(1, from_left, piece).start()

        @pl.when(takes_right & moved)
        def _():
            hop(0, from_right, piece).wait_recv()

            @pl.when(goes_left(piece))
            def _():
                hop(0, from_right, piece).start()

        @pl.loop(0, 2)
        def _(side):
            @pl.when(((side == 0) & takes_left) | ((side == 1) & takes_right & moved))
            def _():
                multiply(me + (2 * side - 1) * back, piece)

    give = pltpu.make_async_remote_copy(
        src_ref=t_ref.at[:, pl.ds(main, t_tail.shape[1])],
        dst_ref=t_tail,
        send_sem=give_sem.at[0],
        recv_sem=give_sem.at[1],
        device_id={"loop": jnp.where(me == 0, 1, n - 2)},
        device_id_type=MESH,
    ) if tail else None

    acc[...] = jnp.zeros_like(acc)
    load_q.wait()
    pl.semaphore_wait(barrier, has_left.astype(jnp.int32) + nf - 1)

    @pl.when(has_left)
    def _():
        pl.semaphore_signal(ready_sem, inc=1, device_id={"loop": me - 1}, device_id_type=MESH)

        @pl.loop(0, pieces)
        def _(piece):
            hop(0, me, piece).start()

    if tail:
        @pl.when(goes_left(None))
        def _():
            hop(0, me, None).start()

    @pl.when(has_right)
    def _():
        pl.semaphore_wait(ready_sem, 1)

        @pl.loop(0, pieces)
        def _(piece):
            hop(1, me, piece).start()

    if tail:
        @pl.when(goes_right(None))
        def _():
            hop(1, me, None).start()

    load_t.wait()
    if tail:
        @pl.when(is_end)
        def _():
            give.start()

    load_c.wait()
    inv_ref[...] = 1.0 / (damping_term + c_ref[...])

    @pl.loop(0, n)
    def _(back):
        @pl.loop(0, pieces)
        def _(piece):
            arrive(back, piece)

        if tail:
            arrive(back, None)

    turned = acc[...].T
    for k in range(nf):
        part[k] = turned[k * own_rows:(k + 1) * own_rows, 0:part.shape[2]]

    shares = []
    for k in range(1, nf):
        peer = lax.rem(f + k, nf)
        share = pltpu.make_async_remote_copy(
            src_ref=part.at[peer],
            dst_ref=red.at[k - 1],
            send_sem=red_send.at[k - 1],
            recv_sem=red_recv.at[k - 1],
            device_id={"feat": peer},
            device_id_type=MESH,
        )
        share.start()
        shares.append(share)

    tail_shares = []
    if tail:
        for k in range(nf):
            peer = lax.rem(f + k, nf)
            tail_shares.append(pltpu.make_async_remote_copy(
                src_ref=tail_part.at[peer],
                dst_ref=tail_red.at[k],
                send_sem=tail_send.at[k],
                recv_sem=tail_recv.at[k],
                device_id={"feat": peer, "loop": jnp.where(me == 1, 0, n - 1)},
                device_id_type=MESH,
            ))

        @pl.when(is_helper)
        def _():
            give.wait_recv()
            tail_acc[...] = jnp.zeros_like(tail_acc)
            wide = math.gcd(tail, 512)

            @pl.loop(0, tail // wide)
            def _(step):
                at = pl.ds(pl.multiple_of(step * wide, 128), wide)
                tail_acc[...] += lax.dot_general(
                    t_tail[:, at], p_tail[:, at].astype(jnp.bfloat16), (((1,), (1,)), ((), ())),
                    preferred_element_type=jnp.float32,
                )

            for k in range(nf):
                tail_part[k] = tail_acc[k * own_rows:(k + 1) * own_rows, :]
            for share in tail_shares:
                share.start()

    @pl.loop(0, n)
    def _(block):
        def sent(piece):
            @pl.when(goes_right(piece) & (block <= me))
            def _():
                hop(1, block, piece).wait_send()

            @pl.when(goes_left(piece) & (block >= me))
            def _():
                hop(0, block, piece).wait_send()

        @pl.loop(0, pieces)
        def _(piece):
            sent(piece)

        if tail:
            sent(None)

    load_count.wait()
    live = f * own_rows + lax.broadcasted_iota(jnp.int32, out_ref.shape, 0) < count_ref[0]
    total = part[f]
    for k in range(1, nf):
        shares[k - 1].wait_recv()
        total = total + red[k - 1]
    out_ref[...] = jnp.where(live, total, 0.0)
    if tail:
        @pl.when(is_end)
        def _():
            more = jnp.zeros_like(total)
            for k in range(nf):
                tail_shares[k].wait_recv()
                more = more + tail_red[k]
            out_ref[...] = jnp.where(live, total + more, 0.0)
            give.wait_send()

        @pl.when(is_helper)
        def _():
            for share in tail_shares:
                share.wait_send()
    for share in shares:
        share.wait_send()


def on_device(n, nf, train_grads, query_grads, curvature, row_counts):
    rows, width = train_grads.shape
    q_rows = query_grads.shape[0]
    queries = n * q_rows
    pieces = max(1, 16 // n)
    unit = 128 * pieces
    tail = width - width * 27 // 32 // unit * unit if n >= 4 else 0
    padded = -(-queries // 128) * 128
    lanes = -(-rows // 128) * 128
    hbm = pl.BlockSpec(memory_space=pltpu.HBM)
    return pl.pallas_call(
        functools.partial(kernel, n, nf, pieces, tail),
        out_shape=pltpu.VMEM((rows // nf, queries), jnp.float32),
        in_specs=[hbm] * 4,
        out_specs=pl.BlockSpec(memory_space=pltpu.VMEM),
        scratch_shapes=[
            pltpu.VMEM((n, q_rows, width), jnp.bfloat16),
            pltpu.VMEM((rows, width), jnp.bfloat16),
            pltpu.SMEM((1,), jnp.int32),
            pltpu.VMEM((1, width), jnp.float32),
            pltpu.VMEM((1, width), jnp.float32),
            pltpu.VMEM((padded, lanes), jnp.float32),
            pltpu.VMEM((nf, rows // nf, queries), jnp.float32),
            pltpu.VMEM((nf - 1, rows // nf, queries), jnp.float32),
            pltpu.VMEM((rows, tail or 128), jnp.bfloat16),
            pltpu.VMEM((queries, tail or 128), jnp.float32),
            pltpu.VMEM((rows, queries), jnp.float32),
            pltpu.VMEM((nf, rows // nf, queries), jnp.float32),
            pltpu.VMEM((nf, rows // nf, queries), jnp.float32),
            pltpu.SemaphoreType.DMA((4,)),
            pltpu.SemaphoreType.DMA((n * (pieces + 1),)),
            pltpu.SemaphoreType.DMA((2, n * (pieces + 1))),
            pltpu.SemaphoreType.DMA((nf - 1,)),
            pltpu.SemaphoreType.DMA((nf - 1,)),
            pltpu.SemaphoreType.DMA((2,)),
            pltpu.SemaphoreType.DMA((nf,)),
            pltpu.SemaphoreType.DMA((nf,)),
            pltpu.SemaphoreType.REGULAR,
        ],
        compiler_params=pltpu.CompilerParams(collective_id=0, has_side_effects=True),
    )(train_grads, query_grads, curvature.reshape(1, width), row_counts)


def solution(mesh):
    placed = (
        P(("groups", "loop"), "feat"),
        P(("groups", "loop"), "feat"),
        P("feat"),
        P(("groups", "loop")),
    )
    return jax.shard_map(
        functools.partial(on_device, mesh.shape["loop"], mesh.shape["feat"]),
        mesh=mesh,
        in_specs=placed,
        out_specs=P(("groups", "loop", "feat"), None),
        check_vma=False,
    )
```

```python
import functools
import math

import jax
import jax.numpy as jnp
from jax import lax
from jax.experimental import pallas as pl
from jax.experimental.pallas import tpu as pltpu
from jax.sharding import PartitionSpec as P

MESH = pl.DeviceIdType.MESH
damping_term = 0.1


def kernel(
    n, nf, pieces, tail,
    t_hbm, q_hbm, c_hbm, count_hbm, out_ref,
    gath, t_ref, count_ref, c_ref, inv_ref, acc, part, red, t_tail, p_tail, tail_acc, tail_part, tail_red,
    local_sem, recv_sem, send_sem, red_recv, red_send, give_sem, tail_recv, tail_send, ready_sem,
):
    me, f = lax.axis_index("loop"), lax.axis_index("feat")
    rows, width = t_ref.shape
    own_rows = rows // nf
    q_rows = gath.shape[1]
    main = width - tail
    cols = main // pieces
    stride = pieces + 1
    has_left, has_right = me > 0, me < n - 1
    is_end = (me == 0) | (me == n - 1)
    is_helper = (me == 1) | (me == n - 2)

    load_q = pltpu.make_async_copy(q_hbm, gath.at[me], local_sem.at[0])
    load_c = pltpu.make_async_copy(c_hbm, c_ref, local_sem.at[1])
    load_t = pltpu.make_async_copy(t_hbm, t_ref, local_sem.at[2])
    load_count = pltpu.make_async_copy(count_hbm, count_ref, local_sem.at[3])
    load_q.start()

    barrier = pltpu.get_barrier_semaphore()

    @pl.when(has_right)
    def _():
        pl.semaphore_signal(barrier, inc=1, device_id={"loop": me + 1}, device_id_type=MESH)

    for k in range(1, nf):
        pl.semaphore_signal(
            barrier, inc=1, device_id={"feat": lax.rem(f + k, nf)}, device_id_type=MESH
        )
    load_c.start()
    load_t.start()
    load_count.start()

    def columns(piece):
        if piece is None:
            return pl.ds(main, tail)
        return pl.ds(pl.multiple_of(piece * cols, 128), cols)

    def hop(way, block, piece):
        span = gath.at[block, :, columns(piece)]
        at = block * stride + (pieces if piece is None else piece)
        return pltpu.make_async_remote_copy(
            src_ref=span,
            dst_ref=span,
            send_sem=send_sem.at[way, at],
            recv_sem=recv_sem.at[at],
            device_id={"loop": jnp.clip(me + (2 * way - 1), 0, n - 1)},
            device_id_type=MESH,
        )

    def goes_right(piece):
        return has_right if piece is not None else me < n - 2

    def goes_left(piece):
        return has_left if piece is not None else me > 1

    def multiply(block, piece):
        start, size = (main, tail) if piece is None else (piece * cols, cols)
        here = pl.ds(pl.multiple_of(block * q_rows, q_rows), q_rows)
        wide = size // 2 if size % 256 == 0 else size

        @pl.loop(0, size // wide)
        def _(step):
            at = pl.ds(pl.multiple_of(start + step * wide, 128), wide)
            exact = gath[block, :, at].astype(jnp.float32) * inv_ref[:, at]
            acc[here, 0:rows] += lax.dot_general(
                exact.astype(jnp.bfloat16), t_ref[:, at], (((1,), (1,)), ((), ())),
                preferred_element_type=jnp.float32,
            )
            if piece is None:
                p_tail[here, pl.ds(pl.multiple_of(step * wide, 128), wide)] = exact

    def arrive(back, piece):
        from_left, from_right = me - back, me + back
        takes_left, takes_right = from_left >= 0, from_right < n
        if piece is None:
            inner = jnp.logical_not(is_end)
            takes_left, takes_right = takes_left & inner, takes_right & inner
        moved = back > 0

        @pl.when(takes_right & moved)
        def _():
            hop(0, from_right, piece).wait_recv()

            @pl.when(goes_left(piece))
            def _():
                hop(0, from_right, piece).start()

        @pl.when(takes_left & moved)
        def _():
            hop(1, from_left, piece).wait_recv()

            @pl.when(goes_right(piece))
            def _():
                hop(1, from_left, piece).start()

        @pl.loop(0, 2)
        def _(side):
            @pl.when(((side == 0) & takes_left) | ((side == 1) & takes_right & moved))
            def _():
                multiply(me + (2 * side - 1) * back, piece)

    give = pltpu.make_async_remote_copy(
        src_ref=t_ref.at[:, pl.ds(main, t_tail.shape[1])],
        dst_ref=t_tail,
        send_sem=give_sem.at[0],
        recv_sem=give_sem.at[1],
        device_id={"loop": jnp.where(me == 0, 1, n - 2)},
        device_id_type=MESH,
    ) if tail else None

    acc[...] = jnp.zeros_like(acc)
    load_q.wait()
    pl.semaphore_wait(barrier, has_left.astype(jnp.int32) + nf - 1)

    @pl.when(has_left)
    def _():
        pl.semaphore_signal(ready_sem, inc=1, device_id={"loop": me - 1}, device_id_type=MESH)

        @pl.loop(0, pieces)
        def _(piece):
            hop(0, me, piece).start()

    if tail:
        @pl.when(goes_left(None))
        def _():
            hop(0, me, None).start()

    @pl.when(has_right)
    def _():
        pl.semaphore_wait(ready_sem, 1)

        @pl.loop(0, pieces)
        def _(piece):
            hop(1, me, piece).start()

    if tail:
        @pl.when(goes_right(None))
        def _():
            hop(1, me, None).start()

    load_t.wait()
    if tail:
        @pl.when(is_end)
        def _():
            give.start()

    load_c.wait()
    inv_ref[...] = 1.0 / (damping_term + c_ref[...])

    @pl.loop(0, n)
    def _(back):
        @pl.loop(0, pieces)
        def _(piece):
            arrive(back, piece)

        if tail:
            arrive(back, None)

    turned = acc[...].T
    for k in range(nf):
        part[k] = turned[k * own_rows:(k + 1) * own_rows, 0:part.shape[2]]

    shares = []
    for k in range(1, nf):
        peer = lax.rem(f + k, nf)
        share = pltpu.make_async_remote_copy(
            src_ref=part.at[peer],
            dst_ref=red.at[k - 1],
            send_sem=red_send.at[k - 1],
            recv_sem=red_recv.at[k - 1],
            device_id={"feat": peer},
            device_id_type=MESH,
        )
        share.start()
        shares.append(share)

    tail_shares = []
    if tail:
        for k in range(nf):
            peer = lax.rem(f + k, nf)
            tail_shares.append(pltpu.make_async_remote_copy(
                src_ref=tail_part.at[peer],
                dst_ref=tail_red.at[k],
                send_sem=tail_send.at[k],
                recv_sem=tail_recv.at[k],
                device_id={"feat": peer, "loop": jnp.where(me == 1, 0, n - 1)},
                device_id_type=MESH,
            ))

        @pl.when(is_helper)
        def _():
            give.wait_recv()
            tail_acc[...] = jnp.zeros_like(tail_acc)
            wide = math.gcd(tail, 512)

            @pl.loop(0, tail // wide)
            def _(step):
                at = pl.ds(pl.multiple_of(step * wide, 128), wide)
                tail_acc[...] += lax.dot_general(
                    t_tail[:, at], p_tail[:, at].astype(jnp.bfloat16), (((1,), (1,)), ((), ())),
                    preferred_element_type=jnp.float32,
                )

            for k in range(nf):
                tail_part[k] = tail_acc[k * own_rows:(k + 1) * own_rows, :]
            for share in tail_shares:
                share.start()

    @pl.loop(0, n)
    def _(block):
        def sent(piece):
            @pl.when(goes_right(piece) & (block <= me))
            def _():
                hop(1, block, piece).wait_send()

            @pl.when(goes_left(piece) & (block >= me))
            def _():
                hop(0, block, piece).wait_send()

        @pl.loop(0, pieces)
        def _(piece):
            sent(piece)

        if tail:
            sent(None)

    load_count.wait()
    live = f * own_rows + lax.broadcasted_iota(jnp.int32, out_ref.shape, 0) < count_ref[0]
    total = part[f]
    for k in range(1, nf):
        shares[k - 1].wait_recv()
        total = total + red[k - 1]
    out_ref[...] = jnp.where(live, total, 0.0)
    if tail:
        @pl.when(is_end)
        def _():
            more = jnp.zeros_like(total)
            for k in range(nf):
                tail_shares[k].wait_recv()
                more = more + tail_red[k]
            out_ref[...] = jnp.where(live, total + more, 0.0)
            give.wait_send()

        @pl.when(is_helper)
        def _():
            for share in tail_shares:
                share.wait_send()
    for share in shares:
        share.wait_send()


def on_device(n, nf, train_grads, query_grads, curvature, row_counts):
    rows, width = train_grads.shape
    q_rows = query_grads.shape[0]
    queries = n * q_rows
    pieces = max(1, 16 // n)
    unit = 128 * pieces
    tail = width - width * 27 // 32 // unit * unit if n >= 4 else 0
    padded = -(-queries // 128) * 128
    lanes = -(-rows // 128) * 128
    hbm = pl.BlockSpec(memory_space=pltpu.HBM)
    return pl.pallas_call(
        functools.partial(kernel, n, nf, pieces, tail),
        out_shape=pltpu.VMEM((rows // nf, queries), jnp.float32),
        in_specs=[hbm] * 4,
        out_specs=pl.BlockSpec(memory_space=pltpu.VMEM),
        scratch_shapes=[
            pltpu.VMEM((n, q_rows, width), jnp.bfloat16),
            pltpu.VMEM((rows, width), jnp.bfloat16),
            pltpu.SMEM((1,), jnp.int32),
            pltpu.VMEM((1, width), jnp.float32),
            pltpu.VMEM((1, width), jnp.float32),
            pltpu.VMEM((padded, lanes), jnp.float32),
            pltpu.VMEM((nf, rows // nf, queries), jnp.float32),
            pltpu.VMEM((nf - 1, rows // nf, queries), jnp.float32),
            pltpu.VMEM((rows, tail or 128), jnp.bfloat16),
            pltpu.VMEM((queries, tail or 128), jnp.float32),
            pltpu.VMEM((rows, queries), jnp.float32),
            pltpu.VMEM((nf, rows // nf, queries), jnp.float32),
            pltpu.VMEM((nf, rows // nf, queries), jnp.float32),
            pltpu.SemaphoreType.DMA((4,)),
            pltpu.SemaphoreType.DMA((n * (pieces + 1),)),
            pltpu.SemaphoreType.DMA((2, n * (pieces + 1))),
            pltpu.SemaphoreType.DMA((nf - 1,)),
            pltpu.SemaphoreType.DMA((nf - 1,)),
            pltpu.SemaphoreType.DMA((2,)),
            pltpu.SemaphoreType.DMA((nf,)),
            pltpu.SemaphoreType.DMA((nf,)),
            pltpu.SemaphoreType.REGULAR,
        ],
        compiler_params=pltpu.CompilerParams(collective_id=0, has_side_effects=True),
    )(train_grads, query_grads, curvature.reshape(1, width), row_counts)


def solution(mesh):
    placed = (
        P(("groups", "loop"), "feat"),
        P(("groups", "loop"), "feat"),
        P("feat"),
        P(("groups", "loop")),
    )
    return jax.shard_map(
        functools.partial(on_device, mesh.shape["loop"], mesh.shape["feat"]),
        mesh=mesh,
        in_specs=placed,
        out_specs=P(("groups", "loop", "feat"), None),
        check_vma=False,
    )
```
